32 devices in a mesh: bank: 8 (over z, y), zero: 4 (over x, core).
Axes of the slice: x: 2, y: 2, z: 4, core: 2. Of those that a mesh axis runs over, the one named last changes fastest.
Arguments:
- w_gate: float32 [64, 2048, 1024], P('bank', 'zero'), may hold values from -0.1875 to 0.1875
- avg_gate: float32 [64, 2048, 1024], P('bank', 'zero'), may hold values from -0.125 to 0.125
- w_up: float32 [64, 2048, 1024], P('bank', 'zero'), may hold values from -0.1875 to 0.1875
- avg_up: float32 [64, 2048, 1024], P('bank', 'zero'), may hold values from -0.125 to 0.125
- mix_share: float32 [64], P('bank'), may hold values from 0.2 to 0.8
- router_weight: float32 [2048, 64], P('zero', 'bank'), may hold values from -0.125 to 0.125
- router_gain: float32 [2048], P('zero'), may hold values from 0.25 to 1.75
Outputs:
- serve_gate: bfloat16 [64, 2048, 1024], P('bank')
- serve_up: bfloat16 [64, 2048, 1024], P('bank')
- scale_gate: float32 [64, 1024], P('bank')
- scale_up: float32 [64, 1024], P('bank')
- serve_router: bfloat16 [2048, 64], replicated
The draws below stay inside these ranges and needn't reach their ends.
All inputs are finite; a program needn't handle non-finite values.
Results may differ from the reference program's by a relative error of at most 0.001.
Values may be sent and summed in bfloat16 or wider, within the bound.
A program may use at most 256 MiB of HBM per device.

```python
import jax
import jax.numpy as jnp
from jax import lax

EXPERTS = 64
D_MODEL = 2048
D_EXPERT = 1024


def spiked(values, rng, source, target, blocks, factor):
    owner, partner = [(jnp.arange(values.shape[axis_at]) // (values.shape[axis_at] // blocks)).reshape([-1 if axis == axis_at else 1 for axis in range(values.ndim)]) for axis_at in (source, target)]
    chosen = jax.random.permutation(rng, blocks)[partner]
    strong = (owner == chosen) | (owner == (partner + blocks // 2) % blocks)
    return jnp.where(strong, factor * values, values)


def block_levels(own_key, dims, shards, low, high):
    gain, own = 1.0, jax.random.fold_in(own_key, 6)
    for axis_at, parts in shards:
        draws = jnp.exp(jax.random.uniform(jax.random.fold_in(own, axis_at), (parts,), jnp.float32, low / len(shards), high / len(shards)))
        gain = gain * jnp.repeat(draws, dims[axis_at] // parts).reshape([-1 if axis == axis_at else 1 for axis in range(len(dims))])
    return gain


def scatter_about(key, shape, width, bound, split=(), kind=jnp.bfloat16):
    level = block_levels(key, shape, split, -0.22, 0.18) if split else 1.0
    array = jax.random.normal(key, shape, jnp.float32) * width * level
    return jnp.minimum(jnp.maximum(array, -bound), bound).astype(kind)


def noise_with(stream_key, extent, spread, reach, pieces, heavy, dtype=jnp.bfloat16):
    values = spread * jax.random.normal(stream_key, extent, jnp.float32)
    if pieces:
        values = values * block_levels(stream_key, extent, pieces, -0.22, 0.18)
    return jnp.clip(spiked(values, jax.random.fold_in(stream_key, 3), *heavy), -reach, reach).astype(dtype)


def setup_inputs(seed: int = 0) -> dict:
    splits = jax.random.split(jax.random.key(seed), 8)
    return {
        "w_gate": noise_with(splits[0], (EXPERTS, D_MODEL, D_EXPERT), D_MODEL ** -0.5, 0.1875, ((0, 8), (1, 4)), (1, 2, 4, 2.0), jnp.float32),
        "avg_gate": scatter_about(splits[1], (EXPERTS, D_MODEL, D_EXPERT), D_MODEL ** -0.5, 0.125, ((0, 8), (1, 4)), jnp.float32),
        "w_up": noise_with(splits[2], (EXPERTS, D_MODEL, D_EXPERT), D_MODEL ** -0.5, 0.1875, ((0, 8), (1, 4)), (1, 2, 4, 2.0), jnp.float32),
        "avg_up": scatter_about(splits[3], (EXPERTS, D_MODEL, D_EXPERT), D_MODEL ** -0.5, 0.125, ((0, 8), (1, 4)), jnp.float32),
        "mix_share": jnp.clip(0.2 + 0.6 * jax.random.uniform(splits[4], (EXPERTS,), jnp.float32) ** block_levels(splits[4], (EXPERTS,), ((0, 8),), -0.2, 0.2), 0.2, 0.8),
        "router_weight": scatter_about(splits[5], (D_MODEL, EXPERTS), D_MODEL ** -0.5, 0.125, ((0, 4), (1, 8)), jnp.float32),
        "router_gain": jnp.clip(1.0 + 0.15 * jax.random.normal(splits[6], (D_MODEL,), jnp.float32), 0.25, 1.75),
    }


def reference(w_gate, avg_gate, w_up, avg_up, mix_share, router_weight, router_gain):
    fresh_gate = mix_share[:, None, None] * w_gate + (1.0 - mix_share[:, None, None]) * avg_gate
    fresh_up = mix_share[:, None, None] * w_up + (1.0 - mix_share[:, None, None]) * avg_up
    scale_gate = jnp.sqrt(lax.optimization_barrier(jnp.sum(fresh_gate * fresh_gate, axis=1)))
    serve_gate = (fresh_gate / jnp.expand_dims(scale_gate, 1)).astype(jnp.bfloat16)
    scale_up = jnp.sqrt(lax.optimization_barrier(jnp.sum(fresh_up * fresh_up, axis=1)))
    serve_up = (fresh_up / jnp.expand_dims(scale_up, 1)).astype(jnp.bfloat16)
    serve_router = (router_weight * router_gain[:, None]).astype(jnp.bfloat16)
    return (serve_gate, serve_up, scale_gate, scale_up, serve_router)
```

```python
import jax
import jax.numpy as jnp
from jax import lax
from jax.experimental import pallas as pl
from jax.sharding import PartitionSpec as P


def copy_body(piece, *refs):
    refs[-1][...] = piece[...]


def place(piece, out, shape, start):
    count, rows, columns = piece.shape
    specs = [pl.BlockSpec((1, rows, columns), lambda e: (e, 0, 0))]
    operands = [piece]
    aliases = {}
    if out is not None:
        specs.append(pl.BlockSpec(memory_space=pl.ANY))
        operands.append(out)
        aliases = {1: 0}
    size = piece.size * piece.dtype.itemsize
    return pl.pallas_call(
        copy_body,
        grid=(count,),
        in_specs=specs,
        out_specs=pl.BlockSpec((1, rows, columns), lambda e: (e + start, 0, 0)),
        out_shape=jax.ShapeDtypeStruct(shape, piece.dtype),
        input_output_aliases=aliases,
        cost_estimate=pl.CostEstimate(flops=0, bytes_accessed=2 * size, transcendentals=0),
    )(*operands)


def narrow(first, second, share):
    fresh = share[:, None, None] * first + (1.0 - share[:, None, None]) * second
    parts = lax.all_gather(jnp.sum(fresh * fresh, axis=1), "zero", axis=0)
    scale = jnp.sqrt(jnp.sum(parts, axis=0))
    return scale, (fresh / jnp.expand_dims(scale, 1)).astype(jnp.bfloat16)


def local(w_gate, avg_gate, w_up, avg_up, mix_share, router_weight, router_gain):
    scale_gate, narrow_gate = narrow(w_gate, avg_gate, mix_share)
    w_up, avg_up, router_weight, narrow_gate = lax.optimization_barrier(
        (w_up, avg_up, router_weight, narrow_gate)
    )
    wide_gate = lax.all_gather(narrow_gate, "zero", axis=1, tiled=True)
    scale_up, narrow_up = narrow(w_up, avg_up, mix_share)
    experts = narrow_up.shape[0]
    last = experts // 4
    cuts = [0, experts - last, experts] if last else [0, experts]
    wide_up = []
    for a, b in zip(cuts, cuts[1:]):
        wide_up.append(lax.all_gather(narrow_up[a:b], "zero", axis=1, tiled=True))
    serve_gate = place(wide_gate, None, wide_gate.shape, 0)
    serve_up = None
    for a, piece in zip(cuts, wide_up):
        serve_up = place(piece, serve_up, wide_gate.shape, a)
    part_router = (router_weight * router_gain[:, None]).astype(jnp.bfloat16)
    row_router = lax.all_gather(part_router, "zero", axis=0, tiled=True)
    serve_router = lax.all_gather(row_router, "bank", axis=1, tiled=True)
    return (serve_gate, serve_up, scale_gate, scale_up, serve_router)


def solution(mesh):
    placed = (
        P("bank", "zero", None),
        P("bank", "zero", None),
        P("bank", "zero", None),
        P("bank", "zero", None),
        P("bank"),
        P("zero", "bank"),
        P("zero"),
    )
    return jax.shard_map(
        local,
        mesh=mesh,
        in_specs=placed,
        out_specs=(
            P("bank", None, None),
            P("bank", None, None),
            P("bank", None),
            P("bank", None),
            P(),
        ),
        check_vma=False,
    )
```
